256 devices in a mesh: node: 16 (over z, core), group: 16 (over x, y).
Axes of the slice: x: 4, y: 4, z: 8, core: 2. Of those that a mesh axis runs over, the one named last changes fastest.
Arguments:
- gradient: bfloat16 [16, 16, 1024, 1024], P('node', 'group'), may hold values from -60 to 60
- momentum: float32 [1024, 1024], replicated, may hold values from -6 to 6
- variance: float32 [1024, 1024], replicated, may hold values from 0.004 to 0.4
- params: float32 [1024, 1024], replicated, may hold values from -6 to 6
- worker_error: float32 [16, 16, 1024, 1024], P('node', 'group'), may hold values from -18 to 18, as said below
- server_error: float32 [16, 1024, 1024], P('group', 'node'), may hold values from -12 to 12, as said below
- group_worker_error: float32 [16, 1024, 1024], P('group', 'node'), may hold values from -12 to 12, as said below
- group_server_error: float32 [1024, 1024], P(('node', 'group')), may hold values from -12 to 12, as said below
Outputs:
- new_params: float32 [1024, 1024], replicated
- new_momentum: float32 [1024, 1024], replicated
- new_worker_error: float32 [16, 16, 1024, 1024], P('node', 'group')
- new_server_error: float32 [16, 1024, 1024], P('group', 'node')
- new_group_worker_error: float32 [16, 1024, 1024], P('group', 'node')
- new_group_server_error: float32 [1024, 1024], P(('node', 'group'))
The draws below stay inside these ranges and needn't reach their ends.
Inputs may be any that keep to these rules, and one draw needn't show every extreme that they name: `worker_error`: no entry of local has magnitude under 0.005. No entry of group_mean + server_error has magnitude under 0.005. No entry of group_q + group_worker_error has magnitude under 0.005. No entry of total_mean + group_server_error has magnitude under 0.005.
All inputs are finite; a program needn't handle non-finite values.
Results may differ from the reference program's by a relative error of at most 0.0003.
Values sent between devices are 32-bit elements; how exact they have to be, the bound alone decides.
A program may use at most 128 MiB of HBM per device.

```python
import math
import jax
import jax.numpy as jnp
from jax import lax

D = 1024
PIECE_ROWS = 4
ROWS = 1024
N_NODE = 16
N_GROUP = 16


def compress_draw(values):
    scale = jnp.mean(jnp.abs(values), axis=-1, keepdims=True)
    return scale * jnp.sign(values)


def signed_draw(key, shape, lower, upper):
    first_key, second_key = jax.random.split(key)
    magnitude = jax.random.uniform(first_key, shape, jnp.float32, lower, upper)
    flips = jax.random.bernoulli(second_key, 0.5, shape)
    return jnp.where(flips, magnitude, -magnitude)


def leaning_target(key, shape, leaning):
    first_key, second_key = jax.random.split(key)
    magnitude = jax.random.uniform(first_key, shape, jnp.float32, 0.1, 0.6)
    agrees = jax.random.bernoulli(second_key, 0.75, shape)
    return jnp.where(agrees, 1.0, -1.0) * leaning * magnitude


def joint_state(key):
    total_rows = PIECE_ROWS * N_NODE * N_GROUP
    base = jax.random.fold_in(key, 101)
    keys = [jax.random.fold_in(base, index) for index in range(8)]
    momentum = jax.random.uniform(keys[2], (total_rows, D), jnp.float32, -0.6, 0.6)
    leaning = jnp.where(momentum >= 0.0, 1.0, -1.0)
    gradient = signed_draw(keys[3], (N_NODE, N_GROUP, total_rows, D), 2.0, 6.0)
    gradient = gradient.astype(jnp.bfloat16)
    moved = 0.9 * momentum + 0.1 * gradient.astype(jnp.float32)
    local_target = leaning_target(keys[4], (N_NODE, N_GROUP, total_rows, D), leaning)
    worker_error = local_target - moved
    first = compress_draw(moved + worker_error)
    group_mean = jnp.sum(first, axis=0) / N_NODE
    server_target = leaning_target(keys[5], (N_GROUP, total_rows, D), leaning)
    server_error = server_target - group_mean
    group_q = compress_draw(group_mean + server_error)
    second_target = leaning_target(keys[6], (N_GROUP, total_rows, D), leaning)
    group_worker_error = second_target - group_q
    second = compress_draw(group_q + group_worker_error)
    total_mean = jnp.sum(second, axis=0) / N_GROUP
    last_target = leaning_target(keys[7], (total_rows, D), leaning)
    group_server_error = last_target - total_mean
    return (momentum, gradient, worker_error, server_error, group_worker_error, group_server_error)


def draw_gradient(key, part):
    return joint_state(key)[1]


def draw_momentum(key, part):
    return joint_state(key)[0]


def draw_worker_error(key, part):
    return joint_state(key)[2]


def draw_server_error(key, part):
    return joint_state(key)[3]


def draw_group_worker_error(key, part):
    return joint_state(key)[4]


def draw_group_server_error(key, part):
    return joint_state(key)[5]


def bell_draw(rng, dims, scale, most, kind=jnp.bfloat16):
    result = scale * jax.random.normal(rng, dims, jnp.float32)
    return jnp.clip(result, min=-most, max=most).astype(kind)


def setup_inputs(seed: int = 0) -> dict:
    key_list = jax.random.split(jax.random.key(seed), 9)
    return {
        "gradient": draw_gradient(jax.random.fold_in(key_list[8], 71), 0),
        "momentum": draw_momentum(jax.random.fold_in(key_list[8], 71), 0),
        "variance": jnp.clip(jnp.exp(jax.random.uniform(key_list[2], (ROWS, D), jnp.float32, math.log(0.004), math.log(0.4))), 0.004, 0.4),
        "params": bell_draw(key_list[3], (ROWS, D), 1.0, 6.0, jnp.float32),
        "worker_error": draw_worker_error(jax.random.fold_in(key_list[8], 71), 0),
        "server_error": draw_server_error(jax.random.fold_in(key_list[8], 71), 0),
        "group_worker_error": draw_group_worker_error(jax.random.fold_in(key_list[8], 71), 0),
        "group_server_error": draw_group_server_error(jax.random.fold_in(key_list[8], 71), 0),
    }


def compress(values):
    scale = lax.optimization_barrier(jnp.mean(jnp.abs(values), axis=-1, keepdims=True))
    packed = scale * jnp.sign(values)
    return (packed, values - packed)

def reference(gradient, momentum, variance, params, worker_error, server_error, group_worker_error, group_server_error):
    local = 0.9 * momentum + 0.1 * gradient.astype(jnp.float32) + worker_error
    first, new_worker_error = compress(local)
    group_mean = lax.optimization_barrier(jnp.sum(first, axis=0)) / N_NODE
    group_q, new_server_error = compress(group_mean + server_error)
    second, new_group_worker_error = compress(group_q + group_worker_error)
    total_mean = lax.optimization_barrier(jnp.sum(second, axis=0)) / N_GROUP
    new_momentum, new_group_server_error = compress(total_mean + group_server_error)
    new_params = params - 0.05 * new_momentum / (jnp.sqrt(variance) + 1e-08)
    return (new_params, new_momentum, new_worker_error, new_server_error, new_group_worker_error, new_group_server_error)
```

```python
import functools

import jax
import jax.numpy as jnp
from jax import lax
from jax.experimental import pallas as pl
from jax.experimental.pallas import tpu as pltpu
from jax.sharding import PartitionSpec as P

MESH = pl.DeviceIdType.MESH
NZ, NX, NY = 8, 4, 4
SHARD = 64
HALF = 32
WIDTH = 1024
PIECE = (8, 512)
OFFSETS = (4, -3, 3, -2, 2, -1, 1, 0)
SLOT = {offset: i for i, offset in enumerate(OFFSETS)}
DOWN = ((4, 0), (-3, 1), (-3, 0), (-2, 1), (-2, 0), (-1, 1), (-1, 0))
UP = ((4, 1), (3, 0), (3, 1), (2, 0), (2, 1), (1, 0), (1, 1))
F32 = jnp.float32


def mod(i, n):
    return lax.rem(i + n, n)


def rows_of(start, size):
    return pl.ds(pl.multiple_of(start, size), size)


def compress(values):
    scale = jnp.sum(jnp.abs(values), axis=1, keepdims=True) * (1.0 / WIDTH)
    packed = jnp.where(values >= 0.0, scale, -scale)
    return packed, values - packed


def kernel(
    grad_hbm, mom_hbm, var_hbm, par_hbm, we_hbm, se_hbm, gwe_hbm, gse_hbm,
    new_p, new_m, new_we, new_se, new_gwe, new_gse,
    gbuf, mbuf, webuf, pbuf, vbuf, sebuf, gwebuf, gsebuf,
    own, psend, precv, rbuf, secp, recvg, mp,
    ld_sem, ld2_sem, ps_sem, pr_sem, rs_send, rs_recv, ge_send, ge_recv,
    z_send, z_recv, b_send, b_recv, a_send, a_recv, d_send, d_recv,
):
    n = lax.axis_index("node")
    g = lax.axis_index("group")
    z, c = lax.div(n, 2), lax.rem(n, 2)
    x, y = lax.div(g, NY), lax.rem(g, NY)
    partner = (2 * z + 1 - c, g)
    sent = []

    def zdev(offset):
        return (2 * mod(z + offset, NZ) + c, g)

    def gdev(dx, dy):
        return (n, mod(x + dx, NX) * NY + mod(y + dy, NY))

    def remote(src, dst, ssem, rsem, device):
        copy = pltpu.make_async_remote_copy(
            src_ref=src, dst_ref=dst, send_sem=ssem, recv_sem=rsem,
            device_id=device, device_id_type=MESH,
        )
        return copy

    def send(src, dst, ssem, rsem, device):
        copy = remote(src, dst, ssem, rsem, device)
        copy.start()
        sent.append(copy)

    def arrived(dst, rsem):
        remote(dst, dst, rsem, rsem, partner).wait_recv()

    barrier = pltpu.get_barrier_semaphore()
    friends = [partner]
    friends += [zdev(o) for o in range(1, NZ)]
    friends += [(n, lax.rem(g + o, NX * NY)) for o in range(1, NX * NY)]
    for device in friends:
        pl.semaphore_signal(barrier, inc=1, device_id=device, device_id_type=MESH)

    loads = {}
    for i, offset in enumerate(OFFSETS):
        rows = rows_of(mod(z + offset, NZ) * (2 * SHARD), 2 * SHARD)
        loads[i] = [
            pltpu.make_async_copy(src.at[rows, :], buf.at[i], ld_sem.at[i, k])
            for k, (src, buf) in enumerate(
                ((grad_hbm, gbuf), (mom_hbm, mbuf), (we_hbm, webuf))
            )
        ]
        for load in loads[i]:
            load.start()
    late = [
        pltpu.make_async_copy(src, buf, ld2_sem.at[k])
        for k, (src, buf) in enumerate(
            ((var_hbm, vbuf), (par_hbm, pbuf), (se_hbm, sebuf), (gwe_hbm, gwebuf), (gse_hbm, gsebuf))
        )
    ]
    for load in late:
        load.start()

    def local_part(i, part, dst):
        zb = mod(z + OFFSETS[i], NZ)

        def step(t, carry):
            r = part * SHARD + t * HALF
            at = rows_of(r, HALF)
            local = 0.9 * mbuf[i, at, :] + 0.1 * gbuf[i, at, :].astype(F32) + webuf[i, at, :]
            packed, error = compress(local)
            dst[i, rows_of(t * HALF, HALF), :] = packed
            new_we[rows_of(zb * (2 * SHARD) + r, HALF), :] = error
            return carry

        lax.fori_loop(0, SHARD // HALF, step, 0)

    def local_block(i, first=False):
        for load in loads[i]:
            load.wait()
        local_part(i, 1 - c, psend)
        if first:
            pl.semaphore_wait(barrier, len(friends))
        send(psend.at[i], precv.at[i], ps_sem.at[i], pr_sem.at[i], partner)
        local_part(i, c, own)

    def half_rows(half):
        return pl.ds(half * HALF, HALF)

    def rs_step(direction, s):
        offset, half = (DOWN, UP)[direction][s]
        i, at = SLOT[offset], half_rows(half)
        device = zdev(-1 if direction == 0 else 1)
        dst = rbuf.at[direction, s]
        if s < 2:
            own[i, at, :] = own[i, at, :] + precv[i, at, :]
            src = own.at[i, at, :]
        else:
            src = rbuf.at[direction, s - 2]
            arrived(src, rs_recv.at[direction, s - 2])
            rbuf[direction, s - 2] = rbuf[direction, s - 2] + (own[i, at, :] + precv[i, at, :])
        send(src, dst, rs_send.at[direction, s], rs_recv.at[direction, s], device)

    def partner_here(i):
        arrived(precv.at[i], pr_sem.at[i])

    local_block(0, first=True)
    partner_here(0)
    rs_step(0, 0)
    rs_step(1, 0)
    local_block(1)
    local_block(2)
    partner_here(1)
    rs_step(0, 1)
    partner_here(2)
    rs_step(1, 1)
    for i in range(3, 8):
        local_block(i)
    for load in late:
        load.wait()
    for i in range(3, 8):
        partner_here(i)

    def coefficients(first, count):
        def step(t, carry):
            at = rows_of(t * HALF, HALF)
            vbuf[at, :] = 0.05 / (jnp.sqrt(vbuf[at, :]) + 1e-8)
            return carry

        lax.fori_loop(first, first + count, step, 0)

    for s in range(2, 7):
        rs_step(0, s)
        rs_step(1, s)
        if s < 6:
            coefficients((s - 2) * 8, 8)

    low = lax.broadcasted_iota(jnp.int32, PIECE, 0) < 4
    last = SLOT[0]
    for half, (down_s, up_s) in ((0, (6, 5)), (1, (5, 6))):
        at = half_rows(half)
        arrived(rbuf.at[0, down_s], rs_recv.at[0, down_s])
        arrived(rbuf.at[1, up_s], rs_recv.at[1, up_s])
        total = own[last, at, :] + precv[last, at, :] + rbuf[0, down_s] + rbuf[1, up_s]
        group_q, error = compress(total * (1.0 / 16.0) + sebuf[at, :])
        new_se[at, :] = error
        second, error = compress(group_q + gwebuf[at, :])
        new_gwe[at, :] = error
        for t in range(HALF // 8):
            left, right = second[8 * t : 8 * t + 8, :512], second[8 * t : 8 * t + 8, 512:]
            k = half * 8 + 2 * t
            secp[k] = jnp.where(low, left, pltpu.roll(right, 4, 0))
            secp[k + 1] = jnp.where(low, pltpu.roll(left, 4, 0), right)

    for o in range(1, NX * NY):
        to = lax.rem(g + o, NX * NY)
        send(secp.at[to], recvg.at[g], ge_send.at[o], ge_recv.at[o], (n, to))
    total = secp[g]
    gse = jnp.concatenate([gsebuf[:, :512], gsebuf[:, 512:]], axis=0)
    for o in range(1, NX * NY):
        source = mod(g - o, NX * NY)
        arrived(recvg.at[source], ge_recv.at[o])
        total = total + recvg[source]
    value = total * (1.0 / 16.0) + gse
    sums = jnp.broadcast_to(jnp.sum(jnp.abs(value), axis=1, keepdims=True), PIECE)
    scale = (sums + pltpu.roll(sums, 4, 0)) * (1.0 / WIDTH)
    piece = jnp.where(value >= 0.0, scale, -scale)
    error = value - piece
    new_gse[:, :512] = error[:4]
    new_gse[:, 512:] = error[4:]

    hz, zz = lax.div(z, 4), lax.rem(z, 4)
    az, bz = y + hz * (x - y), x + hz * (y - x)
    mp[c, hz, az, bz, zz] = piece
    mine = mp.at[c, hz, az, bz, zz]
    for o in range(1, NZ):
        send(mine, mine, z_send.at[o], z_recv.at[o], zdev(o))
    for o in range(1, NZ):
        src = mod(z - o, NZ)
        sh, sz = lax.div(src, 4), lax.rem(src, 4)
        sa, sb = y + sh * (x - y), x + sh * (y - x)
        arrived(mp.at[c, sh, sa, sb, sz], z_recv.at[o])

    def block(h, da, db, core):
        a = mod((y, x)[h] + da, 4)
        b = mod((x, y)[h] + db, 4)
        return mp.at[core, h, a, b]

    def adev(h, d):
        return gdev(0, d) if h == 0 else gdev(d, 0)

    def bdev(h, d):
        return gdev(d, 0) if h == 0 else gdev(0, d)

    def a_spread(h, db):
        ref = block(h, 0, db, c)
        for k, d in enumerate((1, -1)):
            send(ref, ref, a_send.at[h, db, k], a_recv.at[h, db, k], adev(h, d))

    def across(h, da, db):
        ref = block(h, da, db, c)
        send(ref, ref, d_send.at[h, da, db], d_recv.at[h, da, db], partner)

    NEAR = (-1, 1)

    for h in range(2):
        ref = block(h, 0, 0, c)
        for k, d in enumerate((1, -1)):
            send(ref, ref, b_send.at[h, k], b_recv.at[h, k], bdev(h, d))
        a_spread(h, 0)
        across(h, 0, 0)
    for h in range(2):
        for k, d in enumerate((1, -1)):
            ref = block(h, 0, -d, c)
            arrived(ref, b_recv.at[h, k])
            part = ref.at[pl.ds(2 * k, 2)]
            send(part, part, b_send.at[h, 2 + k], b_recv.at[h, 2 + k], bdev(h, d))
            a_spread(h, mod(-d, 4) if isinstance(d, int) is False else (-d) % 4)
            across(h, 0, (-d) % 4)

    def a_forward(h, db):
        for k, d in enumerate((1, -1)):
            ref = block(h, -d, db, c)
            arrived(ref, a_recv.at[h, db, k])
            part = ref.at[pl.ds(2 * k, 2)]
            send(part, part, a_send.at[h, db, 2 + k], a_recv.at[h, db, 2 + k], adev(h, d))
            across(h, (-d) % 4, db)

    for h in range(2):
        a_forward(h, 0)
    for h in range(2):
        ref = block(h, 0, 2, c)
        for k in range(2):
            arrived(ref.at[pl.ds(2 * k, 2)], b_recv.at[h, 2 + k])
        a_spread(h, 2)
        across(h, 0, 2)
    for db in (3, 1, 2):
        for h in range(2):
            a_forward(h, db)
    for db in (0, 3, 1, 2):
        for h in range(2):
            ref = block(h, 2, db, c)
            for k in range(2):
                arrived(ref.at[pl.ds(2 * k, 2)], a_recv.at[h, db, 2 + k])
            across(h, 2, db)
    for db in (0, 3, 1, 2):
        for da in (0, 3, 1, 2):
            for h in range(2):
                arrived(block(h, da, db, 1 - c), d_recv.at[h, da, db])

    for h in range(2):

        def step(t, carry):
            core, rest = lax.div(t, 32), lax.rem(t, 32)
            zq, rest = lax.div(rest, 8), lax.rem(rest, 8)
            px, py = lax.div(rest, 2), lax.rem(rest, 2) * 2
            if h == 0:
                even, odd = mp[core, h, py, px, zq], mp[core, h, py + 1, px, zq]
            else:
                even, odd = mp[core, h, px, py, zq], mp[core, h, px, py + 1, zq]
            at = rows_of(((2 * (4 * h + zq) + core) * 8 + rest) * 8, 8)
            left = jnp.where(low, even, pltpu.roll(odd, 4, 0))
            right = jnp.where(low, pltpu.roll(even, 4, 0), odd)
            new_m[at, :512] = left
            new_m[at, 512:] = right
            new_p[at, :512] = pbuf[at, :512] - vbuf[at, :512] * left
            new_p[at, 512:] = pbuf[at, 512:] - vbuf[at, 512:] * right
            return carry

        lax.fori_loop(0, 64, step, 0)

    for copy in sent:
        copy.wait_send()


def body(gradient, momentum, variance, params, worker_error, server_error, group_worker_error, group_server_error):
    vm, dma = pltpu.VMEM, pltpu.SemaphoreType.DMA
    big = (WIDTH, WIDTH)
    outs = pl.pallas_call(
        kernel,
        out_shape=(
            pltpu.VMEM(big, F32),
            pltpu.VMEM(big, F32),
            pltpu.VMEM(big, F32),
            pltpu.VMEM((SHARD, WIDTH), F32),
            pltpu.VMEM((SHARD, WIDTH), F32),
            pltpu.VMEM((4, WIDTH), F32),
        ),
        in_specs=[pl.BlockSpec(memory_space=pltpu.HBM)] * 8,
        out_specs=[pl.BlockSpec(memory_space=pltpu.VMEM)] * 6,
        scratch_shapes=[
            vm((8, 2 * SHARD, WIDTH), jnp.bfloat16),
            vm((8, 2 * SHARD, WIDTH), F32),
            vm((8, 2 * SHARD, WIDTH), F32),
            vm(big, F32),
            vm(big, F32),
            vm((SHARD, WIDTH), F32),
            vm((SHARD, WIDTH), F32),
            vm((4, WIDTH), F32),
            vm((8, SHARD, WIDTH), F32),
            vm((8, SHARD, WIDTH), F32),
            vm((8, SHARD, WIDTH), F32),
            vm((2, 7, HALF, WIDTH), F32),
            vm((16, *PIECE), F32),
            vm((16, *PIECE), F32),
            vm((2, 2, 4, 4, 4, *PIECE), F32),
            dma((8, 3)), dma((5,)), dma((8,)), dma((8,)),
            dma((2, 7)), dma((2, 7)), dma((16,)), dma((16,)),
            dma((8,)), dma((8,)), dma((2, 4)), dma((2, 4)),
            dma((2, 4, 4)), dma((2, 4, 4)), dma((2, 4, 4)), dma((2, 4, 4)),
        ],
        compiler_params=pltpu.CompilerParams(
            collective_id=0, has_side_effects=True, vmem_limit_bytes=50 * 1024 * 1024
        ),
    )(
        gradient[0, 0], momentum, variance, params, worker_error[0, 0],
        server_error[0], group_worker_error[0], group_server_error,
    )
    new_p, new_m, new_we, new_se, new_gwe, new_gse = outs
    return (new_p, new_m, new_we[None, None], new_se[None], new_gwe[None], new_gse)


def solution(mesh):
    split, shard = P("node", "group", None, None), P("group", "node", None)
    piece = P(("node", "group"), None)
    return jax.shard_map(
        body,
        mesh=mesh,
        in_specs=(split, P(), P(), P(), split, shard, shard, piece),
        out_specs=(P(), P(), split, shard, shard, piece),
        check_vma=False,
    )
```
